32 devices in a mesh: row: 8 (over z, x), col: 4 (over y, core).
Axes of the slice: x: 2, y: 2, z: 4, core: 2. Of those that a mesh axis runs over, the one named last changes fastest.
Arguments:
- p_values: bfloat16 [96, 512, 128], P('row', 'col'), may hold values from -0.8984375 to 0.8984375
- p_where: int32 [96, 8], P('row', 'col'), may hold values from 0 to 63, as said below
- p_count: int32 [8, 4], P('row', 'col'), may hold values from 6 to 12, as said below
- h_values: bfloat16 [96, 512, 128], P('row', 'col'), may hold values from -3 to 3
- h_where: int32 [96, 8], P('row', 'col'), may hold values from 0 to 63, as said below
- h_count: int32 [8, 4], P('row', 'col'), may hold values from 6 to 12, as said below
Outputs:
- ph_values: bfloat16 [96, 512, 128], P('row', 'col')
- php_values: bfloat16 [96, 512, 128], P('row', 'col')
- energy: float32 [], replicated
The draws below stay inside these ranges and needn't reach their ends.
Inputs may be any that keep to these rules, and one draw needn't show every extreme that they name: `p_where`: the 12 slots of the device of row index i and column index j name distinct blocks of its own tile: block rows i * 8 to i * 8 + 7 and the j-th of 4 equal ranges of block columns. `h_where`: as for p_where. `p_count`: some device has all 12 slots live. `h_count`: some device has all 12 slots live.
All inputs are finite; a program needn't handle non-finite values.
Results may differ from the reference program's by a relative error of at most 0.0049.
Values may be sent and summed in bfloat16 or wider, within the bound.
A program may use at most 64 MiB of HBM per device.

```python
import jax
import jax.numpy as jnp
from jax import lax

BLK = 128
TILE = 8
CAP = 12
NBLK = 64
N_ROW = 8
N_COL = 4


def tile_coords(key):
    tile_cols = NBLK // N_COL
    keys_all = jax.random.split(key, N_ROW * N_COL)

    def one_tile(tile_key):
        return jax.random.permutation(tile_key, TILE * tile_cols)[:CAP]
    picks = jax.vmap(one_tile)(keys_all).reshape(N_ROW, N_COL, CAP)
    row_base = (jnp.arange(N_ROW, dtype=jnp.int32) * TILE)[:, None, None]
    col_base = (jnp.arange(N_COL, dtype=jnp.int32) * tile_cols)[None, :, None]
    block_rows = picks // tile_cols + row_base
    block_cols = picks % tile_cols + col_base
    stacked = jnp.stack([block_rows, block_cols], axis=-1)
    return jnp.transpose(stacked, (0, 2, 1, 3)).reshape(N_ROW * CAP, N_COL * 2).astype(jnp.int32)


def slot_counts(key):
    low_key, full_key = jax.random.split(key)
    counts = jax.random.randint(low_key, (N_ROW * N_COL,), (CAP + 1) // 2, CAP + 1)
    where_full = jax.random.randint(full_key, (), 0, N_ROW * N_COL)
    return counts.at[where_full].set(CAP).reshape(N_ROW, N_COL).astype(jnp.int32)


def draw_p_where(key, part):
    return tile_coords(jax.random.fold_in(key, 3))


def draw_h_where(key, part):
    return tile_coords(jax.random.fold_in(key, 5))


def draw_p_count(key, part):
    return slot_counts(jax.random.fold_in(key, 7))


def draw_h_count(key, part):
    return slot_counts(jax.random.fold_in(key, 11))


def level_of(own_key, extent, cuts, smallest, top_value):
    loudness = 1.0
    for dim, parts in cuts:
        heights = jax.random.uniform(jax.random.fold_in(jax.random.fold_in(own_key, 6), dim), (parts,), jnp.float32, smallest / len(cuts), top_value / len(cuts))
        loudness = loudness * jnp.repeat(jnp.exp(heights), extent[dim] // parts).reshape((-1,) + (1,) * (len(extent) - 1 - dim))
    return loudness


def gaussian(own_key, shape, deviation, bound, cuts=(), kind=jnp.bfloat16):
    loudness = level_of(own_key, shape, cuts, -0.22, 0.18) if cuts else 1.0
    result = jax.random.normal(own_key, shape, jnp.float32) * deviation * loudness
    return jnp.minimum(jnp.maximum(result, -bound), bound).astype(kind)


def setup_inputs(seed: int = 0) -> dict:
    splits = jax.random.split(jax.random.key(seed), 7)
    return {
        "p_values": gaussian(splits[0], (N_ROW * CAP, N_COL * BLK, BLK), 0.15, 0.8984375, ((0, 8), (1, 4))),
        "p_where": draw_p_where(jax.random.fold_in(splits[6], 71), 0),
        "p_count": draw_p_count(jax.random.fold_in(splits[6], 71), 0),
        "h_values": gaussian(splits[3], (N_ROW * CAP, N_COL * BLK, BLK), 0.5, 3.0, ((0, 8), (1, 4))),
        "h_where": draw_h_where(jax.random.fold_in(splits[6], 71), 0),
        "h_count": draw_h_count(jax.random.fold_in(splits[6], 71), 0),
    }


def index_table(where_arg, count_arg):
    shaped = where_arg.reshape(N_ROW, CAP, N_COL, 2)
    block_rows = shaped[..., 0].reshape(-1)
    block_cols = shaped[..., 1].reshape(-1)
    slot_ids = jnp.arange(CAP, dtype=jnp.int32)[None, :, None]
    live_slots = (slot_ids < count_arg[:, None, :]).reshape(-1)
    flat_ids = jnp.arange(N_ROW * CAP * N_COL, dtype=jnp.int32)
    target_rows = jnp.where(live_slots, block_rows, NBLK).astype(jnp.int32)
    table = jnp.full((NBLK, NBLK), -1, jnp.int32).at[target_rows, block_cols].set(flat_ids, mode="drop")
    return table, block_rows, block_cols, live_slots


def flatten_values(values):
    return values.reshape(N_ROW * CAP, N_COL, BLK, BLK).reshape(-1, BLK, BLK)


def unflatten_values(flat):
    return flat.reshape(N_ROW * CAP, N_COL, BLK, BLK).reshape(N_ROW * CAP, N_COL * BLK, BLK)


def sparse_product(left_flat, left_table, right_flat, right_table, block_rows, block_cols):
    def one_block(coords):
        row_ids = left_table[coords[0], :]
        col_ids = right_table[:, coords[1]]
        left_blocks = jnp.take(left_flat, jnp.maximum(row_ids, 0), axis=0)
        right_blocks = jnp.take(right_flat, jnp.maximum(col_ids, 0), axis=0)
        left_blocks = jnp.where((row_ids >= 0)[:, None, None], left_blocks.astype(jnp.float32), jnp.float32(0.0))
        right_blocks = jnp.where((col_ids >= 0)[:, None, None], right_blocks.astype(jnp.float32), jnp.float32(0.0))
        return jnp.einsum("kxy,kyz->xz", left_blocks, right_blocks)

    return lax.map(one_block, (block_rows, block_cols))


def reference(p_values, p_where, p_count, h_values, h_where, h_count):
    p_table, block_rows, block_cols, live_slots = index_table(p_where, p_count)
    h_table, h_rows, h_cols, h_live = index_table(h_where, h_count)
    p_flat = flatten_values(p_values)
    h_flat = flatten_values(h_values)
    first_sum = sparse_product(p_flat, p_table, h_flat, h_table, block_rows, block_cols)
    first_sum = jnp.where(live_slots[:, None, None], first_sum, jnp.float32(0.0))
    traces = jnp.trace(first_sum, axis1=1, axis2=2)
    energy = jnp.sum(jnp.where(live_slots & (block_rows == block_cols), traces, jnp.float32(0.0)))
    ph_flat = first_sum.astype(jnp.bfloat16)
    second_sum = sparse_product(ph_flat, p_table, p_flat, p_table, block_rows, block_cols)
    second_sum = jnp.where(live_slots[:, None, None], second_sum, jnp.float32(0.0))
    php_flat = second_sum.astype(jnp.bfloat16)
    return unflatten_values(ph_flat), unflatten_values(php_flat), energy
```

```python
import functools

import jax
import jax.numpy as jnp
from jax import lax
from jax.experimental import pallas as pl
from jax.experimental.pallas import tpu as pltpu
from jax.sharding import PartitionSpec as P

TILE = 8
CHUNKS = 3
IN_FLIGHT = 16
MESH = pl.DeviceIdType.MESH
ANY = pl.BlockSpec(memory_space=pl.ANY)
VMEM = pl.BlockSpec(memory_space=pltpu.VMEM)
SMEM = pl.BlockSpec(memory_space=pltpu.SMEM)


def at_row(r):
    return (r, lax.axis_index("col"))


def at_col(c):
    return (lax.axis_index("row"), c)


def remote(src, dst, send_sem, recv_sem, device):
    return pltpu.make_async_remote_copy(
        src_ref=src,
        dst_ref=dst,
        send_sem=send_sem,
        recv_sem=recv_sem,
        device_id=device,
        device_id_type=MESH,
    )


def greet(rows, cols):
    me_row, me_col = lax.axis_index("row"), lax.axis_index("col")
    barrier = pltpu.get_barrier_semaphore()
    for d in range(1, rows):
        pl.semaphore_signal(
            barrier, inc=1, device_id=at_row((me_row + d) % rows), device_id_type=MESH
        )
    for d in range(1, cols):
        pl.semaphore_signal(
            barrier, inc=1, device_id=at_col((me_col + d) % cols), device_id_type=MESH
        )
    pl.semaphore_wait(barrier, rows + cols - 2)


class ColumnGather:
    def __init__(self, rows, own, out, own_send, own_recv, fwd_send):
        self.rows, self.own, self.out = rows, own, out
        self.sems = own_send, own_recv, fwd_send
        self.inner = 2 if rows % 2 == 0 else 1
        self.outer = rows // self.inner
        slots = own.shape[0]
        self.chunks = CHUNKS if slots % CHUNKS == 0 else 1
        self.size = slots // self.chunks
        self.me = lax.axis_index("row")
        self.x, self.z = self.me % self.inner, self.me // self.inner
        self.pair = self.z * self.inner + (self.inner - 1 - self.x)

    def row_of(self, d):
        return ((self.z + d) % self.outer) * self.inner + self.x

    def part(self, ch):
        return pl.ds(ch * self.size, self.size)

    def send(self, ch, d):
        own_send, recv, _ = self.sems
        target = self.pair if d == 0 else self.row_of(d)
        return remote(
            self.own.at[self.part(ch)],
            self.out.at[self.me, self.part(ch)],
            own_send.at[d, ch],
            recv.at[self.me, ch],
            at_row(target),
        )

    def forward(self, ch, d):
        _, recv, fwd = self.sems
        r = self.row_of(d)
        return remote(
            self.out.at[r, self.part(ch)],
            self.out.at[r, self.part(ch)],
            fwd.at[d, ch],
            recv.at[r, ch],
            at_row(self.pair),
        )

    def arrival(self, ch, r):
        _, recv, fwd = self.sems
        return remote(
            self.out.at[r, self.part(ch)],
            self.out.at[r, self.part(ch)],
            fwd.at[0, ch],
            recv.at[r, ch],
            at_row(self.pair),
        )

    def order(self):
        out = []
        for k in range(1, self.outer):
            d = (k + 1) // 2 if k % 2 else -(k // 2)
            out.append(d % self.outer)
        return out

    def start(self):
        for ch in range(self.chunks):
            if self.inner == 2:
                self.send(ch, 0).start()
            for d in self.order():
                self.send(ch, d).start()

    def relay(self, ch):
        for d in self.order():
            self.arrival(ch, self.row_of(d)).wait_recv()
            if self.inner == 2:
                self.forward(ch, d).start()

    def finish(self):
        for ch in range(self.chunks):
            if self.inner == 2:
                self.arrival(ch, self.pair).wait_recv()
                self.send(ch, 0).wait_send()
            for d in self.order():
                self.send(ch, d).wait_send()
                if self.inner == 2:
                    other = ((self.z + d) % self.outer) * self.inner + (1 - self.x)
                    self.arrival(ch, other).wait_recv()
                    self.forward(ch, d).wait_send()


def col_copies(cols, own, out, send, recv):
    me = lax.axis_index("col")
    made = []
    for d in range(1, cols):
        made.append(
            remote(own, out.at[me], send.at[d], recv.at[d], at_col((me + d) % cols))
        )
    return made


def row_copies(rows, own, out, send, recv):
    me = lax.axis_index("row")
    made = []
    for d in range(1, rows):
        made.append(
            remote(own, out.at[me], send.at[d], recv.at[d], at_row((me + d) % rows))
        )
    return made


def first_gather(
    rows, cols, p_ref, h_ref, meta_ref, prow, hcol, prow_meta, col_meta,
    own_send, own_recv, fwd_send, p_send, p_recv, mc_send, mc_recv, mr_send, mr_recv, local,
):
    me_row, me_col = lax.axis_index("row"), lax.axis_index("col")
    keep = [
        pltpu.make_async_copy(h_ref, hcol.at[me_row], local.at[0]),
        pltpu.make_async_copy(p_ref, prow.at[me_col], local.at[1]),
        pltpu.make_async_copy(meta_ref, prow_meta.at[me_col], local.at[2]),
        pltpu.make_async_copy(meta_ref, col_meta.at[me_row], local.at[3]),
    ]
    greet(rows, cols)
    gather = ColumnGather(rows, h_ref, hcol, own_send, own_recv, fwd_send)
    gather.start()
    across = (
        col_copies(cols, p_ref, prow, p_send, p_recv)
        + col_copies(cols, meta_ref, prow_meta, mc_send, mc_recv)
        + row_copies(rows, meta_ref, col_meta, mr_send, mr_recv)
    )
    for copy in across + keep:
        copy.start()
    for ch in range(gather.chunks):
        gather.relay(ch)
    gather.finish()
    for copy in across + keep:
        copy.wait()


def second_gather(
    rows, cols, p_ref, f_ref, e_ref, frow, pcol, e_out,
    e_cols, e_rows, e_sum,
    own_send, own_recv, fwd_send, p_send, p_recv, ec_send, ec_recv, er_send, er_recv, local,
):
    me_row, me_col = lax.axis_index("row"), lax.axis_index("col")
    keep = [
        pltpu.make_async_copy(p_ref, pcol.at[me_row], local.at[0]),
        pltpu.make_async_copy(f_ref, frow.at[me_col], local.at[1]),
    ]
    greet(rows, cols)
    energies = col_copies(cols, e_ref, e_cols, ec_send, ec_recv)
    for copy in energies:
        copy.start()
    gather = ColumnGather(rows, p_ref, pcol, own_send, own_recv, fwd_send)
    gather.start()
    across = col_copies(cols, f_ref, frow, p_send, p_recv)
    for copy in across + keep:
        copy.start()
    e_cols[me_col] = e_ref[...]
    for copy in energies:
        copy.wait()
    total = e_cols[0]
    for c in range(1, cols):
        total = total + e_cols[c]
    e_sum[...] = total
    e_rows[me_row] = total
    gather.relay(0)
    sums = row_copies(rows, e_sum, e_rows, er_send, er_recv)
    for copy in sums:
        copy.start()
    for ch in range(1, gather.chunks):
        gather.relay(ch)
    for copy in sums:
        copy.wait()
    total = e_rows[0]
    for r in range(1, rows):
        total = total + e_rows[r]
    e_out[...] = total
    gather.finish()
    for copy in across + keep:
        copy.wait()


def block_products(
    rows, cols, right_lane, with_trace, lmeta, rmeta, left, right, *rest
):
    if with_trace:
        out, e_out = rest[:2]
    else:
        e_in, out, e_out = rest[:3]
    acc, lbuf, rbuf, head, nxt, inner, mask, table, ml, mr, ms, sems = rest[-12:]
    slots = out.shape[0]
    i, j = lax.axis_index("row"), lax.axis_index("col")
    nblk = rows * TILE
    tile_cols = nblk // cols
    words = -(-nblk // 32)
    count_lane = 4 * slots
    acc[...] = jnp.zeros_like(acc)

    for t in range(TILE):
        head[t] = -1

    for t in range(tile_cols * words):
        mask[t] = 0

    @pl.loop(0, cols)
    def _(c):
        @pl.loop(0, lmeta[c, 0, count_lane])
        def _(s):
            row = lmeta[c, 0, s] - i * TILE
            idx = c * slots + s
            inner[idx] = lmeta[c, 0, slots + s]
            nxt[idx] = head[row]
            head[row] = idx

    @pl.loop(0, rows)
    def _(r):
        @pl.loop(0, rmeta[r, 0, count_lane + (1 if right_lane else 0)])
        def _(s):
            k = rmeta[r, 0, right_lane + s]
            col = rmeta[r, 0, right_lane + slots + s] - j * tile_cols
            word = col * words + (k >> 5)
            mask[word] = mask[word] | (jnp.int32(1) << (k & 31))
            table[k * tile_cols + col] = r * slots + s

    def find_slot(s, n):
        row = lmeta[j, 0, s] - i * TILE
        col = lmeta[j, 0, slots + s] - j * tile_cols

        def more(state):
            return state[0] >= 0

        def step(state):
            at, n = state
            k = inner[at]
            ml[n] = at
            mr[n] = table[k * tile_cols + col]
            ms[n] = s
            return nxt[at], n + ((mask[col * words + (k >> 5)] >> (k & 31)) & 1)

        return lax.while_loop(more, step, (head[row], n))[1]

    own_count = lmeta[j, 0, count_lane]
    found = lax.fori_loop(0, own_count, find_slot, jnp.int32(0))

    def fetch(base, m):
        a, b = ml[base + m], mr[base + m]
        return (
            pltpu.make_async_copy(left.at[a], lbuf.at[m], sems.at[0, m]),
            pltpu.make_async_copy(right.at[b], rbuf.at[m], sems.at[1, m]),
        )

    @pl.loop(0, (found + IN_FLIGHT - 1) // IN_FLIGHT)
    def _(chunk):
        base = chunk * IN_FLIGHT
        size = jnp.minimum(found - base, IN_FLIGHT)

        @pl.loop(0, size)
        def _(m):
            for copy in fetch(base, m):
                copy.start()

        @pl.loop(0, size)
        def _(m):
            for copy in fetch(base, m):
                copy.wait()
            s = ms[base + m]
            acc[s] += jnp.dot(lbuf[m], rbuf[m], preferred_element_type=jnp.float32)

    out[...] = acc[...].astype(out.dtype)
    if with_trace:
        size = acc.shape[1]
        e_out[...] = jnp.zeros_like(e_out)
        diagonal = lax.broadcasted_iota(jnp.int32, (size, size), 0) == lax.broadcasted_iota(
            jnp.int32, (size, size), 1
        )

        @pl.loop(0, own_count)
        def _(s):
            @pl.when(lmeta[j, 0, s] == lmeta[j, 0, slots + s])
            def _():
                e_out[...] += jnp.sum(jnp.where(diagonal, acc[s], 0.0))
    else:
        e_out[0, 0] = e_in[0, 0]


def per_device(rows, cols, p_values, p_where, p_count, h_values, h_where, h_count):
    slots, size, _ = p_values.shape
    dtype = p_values.dtype
    nblk = rows * TILE
    tile_cols = nblk // cols
    words = -(-nblk // 32)
    meta = jnp.concatenate(
        [p_where[:, 0], p_where[:, 1], h_where[:, 0], h_where[:, 1], p_count[0], h_count[0]]
    )
    meta = jnp.broadcast_to(jnp.pad(meta, (0, 128 - meta.shape[0]))[None, :], (8, 128))
    dma = pltpu.SemaphoreType.DMA
    chunk_sems = [dma((rows, CHUNKS)), dma((rows, CHUNKS)), dma((rows, CHUNKS))]
    col_sems = [dma((cols,)), dma((cols,))]
    row_sems = [dma((rows,)), dma((rows,))]
    tile = (slots, size, size)
    prow, hcol, prow_meta, col_meta = pl.pallas_call(
        functools.partial(first_gather, rows, cols),
        out_shape=[
            jax.ShapeDtypeStruct((cols,) + tile, dtype),
            jax.ShapeDtypeStruct((rows,) + tile, dtype),
            jax.ShapeDtypeStruct((cols, 8, 128), jnp.int32),
            jax.ShapeDtypeStruct((rows, 8, 128), jnp.int32),
        ],
        in_specs=[VMEM] * 3,
        out_specs=[ANY] * 4,
        scratch_shapes=chunk_sems + col_sems + col_sems + row_sems + [dma((4,))],
        compiler_params=pltpu.CompilerParams(collective_id=0, has_side_effects=True),
        name="first_gather",
    )(p_values, h_values, meta)

    def products(right_lane, with_trace, lmeta, rmeta, left, right, *more):
        smem = lambda n: pltpu.SMEM((n,), jnp.int32)
        most = slots * nblk + 1
        return pl.pallas_call(
            functools.partial(block_products, rows, cols, right_lane, with_trace),
            out_shape=[
                jax.ShapeDtypeStruct(tile, dtype),
                jax.ShapeDtypeStruct((8, 128) if with_trace else (1, 1), jnp.float32),
            ],
            in_specs=[SMEM, SMEM, ANY, ANY] + [SMEM] * len(more),
            out_specs=[VMEM, VMEM if with_trace else SMEM],
            scratch_shapes=[
                pltpu.VMEM(tile, jnp.float32),
                pltpu.VMEM((IN_FLIGHT, size, size), dtype),
                pltpu.VMEM((IN_FLIGHT, size, size), dtype),
                smem(TILE),
                smem(cols * slots),
                smem(cols * slots),
                smem(tile_cols * words),
                smem(nblk * tile_cols),
                smem(most),
                smem(most),
                smem(most),
                dma((2, IN_FLIGHT)),
            ],
            name="products",
        )(
            lmeta,
            rmeta,
            left.reshape((cols * slots, size, size)),
            right.reshape((rows * slots, size, size)),
            *more,
        )

    ph_values, part = products(2 * slots, True, prow_meta, col_meta, prow, hcol)
    frow, pcol, energy = pl.pallas_call(
        functools.partial(second_gather, rows, cols),
        out_shape=[
            jax.ShapeDtypeStruct((cols,) + tile, dtype),
            jax.ShapeDtypeStruct((rows,) + tile, dtype),
            jax.ShapeDtypeStruct((8, 128), jnp.float32),
        ],
        in_specs=[VMEM] * 3,
        out_specs=[ANY, ANY, VMEM],
        scratch_shapes=[
            pltpu.VMEM((cols, 8, 128), jnp.float32),
            pltpu.VMEM((rows, 8, 128), jnp.float32),
            pltpu.VMEM((8, 128), jnp.float32),
        ]
        + chunk_sems + col_sems + col_sems + row_sems + [dma((2,))],
        compiler_params=pltpu.CompilerParams(collective_id=1, has_side_effects=True),
        name="second_gather",
    )(p_values, ph_values, part)
    php_values, energy = products(0, False, prow_meta, col_meta, frow, pcol, energy)
    return (ph_values, php_values, energy[0, 0])


def solution(mesh):
    placed = (
        P("row", "col", None),
        P("row", "col"),
        P("row", "col"),
        P("row", "col", None),
        P("row", "col"),
        P("row", "col"),
    )
    return jax.shard_map(
        functools.partial(per_device, mesh.shape["row"], mesh.shape["col"]),
        mesh=mesh,
        in_specs=placed,
        out_specs=(P("row", "col", None), P("row", "col", None), P()),
        check_vma=False,
    )
```

```python
import functools

import jax
import jax.numpy as jnp
from jax import lax
from jax.experimental import pallas as pl
from jax.experimental.pallas import tpu as pltpu
from jax.sharding import PartitionSpec as P

TILE = 8
CHUNKS = 6
IN_FLIGHT = 16
MESH = pl.DeviceIdType.MESH
ANY = pl.BlockSpec(memory_space=pl.ANY)
VMEM = pl.BlockSpec(memory_space=pltpu.VMEM)
SMEM = pl.BlockSpec(memory_space=pltpu.SMEM)


def at_row(r):
    return (r, lax.axis_index("col"))


def at_col(c):
    return (lax.axis_index("row"), c)


def remote(src, dst, send_sem, recv_sem, device):
    return pltpu.make_async_remote_copy(
        src_ref=src,
        dst_ref=dst,
        send_sem=send_sem,
        recv_sem=recv_sem,
        device_id=device,
        device_id_type=MESH,
    )


def greet(rows, cols):
    me_row, me_col = lax.axis_index("row"), lax.axis_index("col")
    barrier = pltpu.get_barrier_semaphore()
    for d in range(1, rows):
        pl.semaphore_signal(
            barrier, inc=1, device_id=at_row((me_row + d) % rows), device_id_type=MESH
        )
    for d in range(1, cols):
        pl.semaphore_signal(
            barrier, inc=1, device_id=at_col((me_col + d) % cols), device_id_type=MESH
        )
    pl.semaphore_wait(barrier, rows + cols - 2)


class ColumnGather:
    def __init__(self, rows, own, land, out, up_send, down_send, x_send, recv, local):
        self.own, self.land, self.out = own, land, out
        self.up_send, self.down_send, self.x_send = up_send, down_send, x_send
        self.recv, self.local = recv, local
        self.inner = 2 if rows % 2 == 0 else 1
        self.outer = rows // self.inner
        self.chunks = recv.shape[1]
        self.size = own.shape[0] // self.chunks
        self.me = lax.axis_index("row")
        self.x, self.z = self.me % self.inner, self.me // self.inner
        self.cross_first = 1 if self.inner == 2 and self.chunks > 1 else 0

    def row(self, z, line):
        return z * self.inner + (self.x if line == 0 else self.inner - 1 - self.x)

    def part(self, ch):
        return pl.ds(ch * self.size, self.size)

    def copy(self, r, ch, own, way):
        sems, target = {
            "up": (self.up_send, self.me + self.inner),
            "down": (self.down_send, self.me - self.inner),
            "x": (self.x_send, self.row(self.z, 1)),
        }[way]
        part = self.part(ch)
        src = self.own.at[part] if own else self.land.at[r, part]
        return remote(src, self.land.at[r, part], sems.at[r, ch], self.recv.at[r, ch], at_row(target))

    def keep(self, r, ch):
        part = self.part(ch)
        return pltpu.make_async_copy(self.land.at[r, part], self.out.at[r, part], self.local.at[r, ch])

    def along(self, r, ch, own, act):
        @pl.when(self.z < self.outer - 1)
        def _():
            act(self.copy(r, ch, own, "up"))

        @pl.when(self.z > 0)
        def _():
            act(self.copy(r, ch, own, "down"))

    def arrive(self, r, ch):
        self.copy(r, ch, False, "x").wait_recv()
        self.keep(r, ch).start()

    def start(self):
        for ch in range(self.chunks):
            if self.inner == 2:
                self.copy(self.me, ch, True, "x").start()
            self.along(self.me, ch, True, lambda copy: copy.start())
        if self.cross_first:
            r = self.row(self.z, 1)
            self.arrive(r, 0)
            self.along(r, 0, False, lambda copy: copy.start())

    def pieces(self):
        lines = [(ch, 0) for ch in range(self.chunks)]
        if self.cross_first:
            lines.insert(1, (0, 1))
        return lines

    def relayed(self, d, side, ch, line, act):
        z = self.z - d if side == 0 else self.z + d
        there = self.z >= d if side == 0 else self.z + d < self.outer
        r = self.row(z, line)

        @pl.when(there)
        def _():
            if act == "start":
                self.arrive(r, ch)
            on = self.z < self.outer - 1 if side == 0 else self.z > 0

            @pl.when(on)
            def _():
                copy = self.copy(r, ch, False, "up" if side == 0 else "down")
                copy.start() if act == "start" else copy.wait_send()

            if self.inner == 2 and ch >= self.cross_first:
                copy = self.copy(r, ch, False, "x")
                copy.start() if act == "start" else copy.wait_send()

    def relay(self, d):
        for ch, line in self.pieces():
            for side in range(2):
                self.relayed(d, side, ch, line, "start")

    def finish(self):
        if self.inner == 2:
            for ch in range(self.cross_first, self.chunks):
                self.arrive(self.row(self.z, 1), ch)
            for d in range(1, self.outer):
                for side in range(2):
                    z = self.z - d if side == 0 else self.z + d
                    there = self.z >= d if side == 0 else self.z + d < self.outer

                    @pl.when(there)
                    def _():
                        for ch in range(self.cross_first, self.chunks):
                            self.arrive(self.row(z, 1), ch)
        for ch in range(self.chunks):
            if self.inner == 2:
                self.copy(self.me, ch, True, "x").wait_send()
            self.along(self.me, ch, True, lambda copy: copy.wait_send())
        if self.cross_first:
            self.along(self.row(self.z, 1), 0, False, lambda copy: copy.wait_send())
        for d in range(1, self.outer):
            for ch, line in self.pieces():
                for side in range(2):
                    self.relayed(d, side, ch, line, "wait")
        for r in range(self.inner * self.outer):
            @pl.when(r != self.me)
            def _():
                for ch in range(self.chunks):
                    self.keep(r, ch).wait()


def col_copies(cols, own, out, send, recv):
    me = lax.axis_index("col")
    made = []
    for d in range(1, cols):
        made.append(
            remote(own, out.at[me], send.at[d], recv.at[d], at_col((me + d) % cols))
        )
    return made


def row_copies(rows, own, out, send, recv):
    me = lax.axis_index("row")
    made = []
    for d in range(1, rows):
        made.append(
            remote(own, out.at[me], send.at[d], recv.at[d], at_row((me + d) % rows))
        )
    return made


def first_gather(
    rows, cols, p_ref, h_ref, meta_ref, prow, hcol, prow_meta, col_meta,
    land, up_send, down_send, x_send, recv, out_sems,
    p_send, p_recv, mc_send, mc_recv, mr_send, mr_recv, local,
):
    me_row, me_col = lax.axis_index("row"), lax.axis_index("col")
    keep = [
        pltpu.make_async_copy(h_ref, hcol.at[me_row], local.at[0]),
        pltpu.make_async_copy(p_ref, prow.at[me_col], local.at[1]),
        pltpu.make_async_copy(meta_ref, prow_meta.at[me_col], local.at[2]),
        pltpu.make_async_copy(meta_ref, col_meta.at[me_row], local.at[3]),
    ]
    greet(rows, cols)
    gather = ColumnGather(
        rows, h_ref, land, hcol, up_send, down_send, x_send, recv, out_sems
    )
    across = (
        col_copies(cols, p_ref, prow, p_send, p_recv)
        + col_copies(cols, meta_ref, prow_meta, mc_send, mc_recv)
        + row_copies(rows, meta_ref, col_meta, mr_send, mr_recv)
    )
    for copy in across + keep:
        copy.start()
    gather.start()
    for d in range(1, gather.outer):
        gather.relay(d)
    gather.finish()
    for copy in across + keep:
        copy.wait()


def second_gather(
    rows, cols, p_ref, f_ref, e_ref, frow, pcol, e_out,
    e_cols, e_rows, e_sum,
    land, up_send, down_send, x_send, recv, out_sems,
    p_send, p_recv, ec_send, ec_recv, er_send, er_recv, local,
):
    me_row, me_col = lax.axis_index("row"), lax.axis_index("col")
    keep = [
        pltpu.make_async_copy(p_ref, pcol.at[me_row], local.at[0]),
        pltpu.make_async_copy(f_ref, frow.at[me_col], local.at[1]),
    ]
    greet(rows, cols)
    energies = col_copies(cols, e_ref, e_cols, ec_send, ec_recv)
    for copy in energies:
        copy.start()
    gather = ColumnGather(
        rows, p_ref, land, pcol, up_send, down_send, x_send, recv, out_sems
    )
    across = col_copies(cols, f_ref, frow, p_send, p_recv)
    for copy in across + keep:
        copy.start()
    gather.start()
    e_cols[me_col] = e_ref[...]
    for copy in energies:
        copy.wait()
    total = e_cols[0]
    for c in range(1, cols):
        total = total + e_cols[c]
    e_sum[...] = total
    e_rows[me_row] = total
    if gather.outer > 1:
        gather.relay(1)
    sums = row_copies(rows, e_sum, e_rows, er_send, er_recv)
    for copy in sums:
        copy.start()
    for d in range(2, gather.outer):
        gather.relay(d)
    for copy in sums:
        copy.wait()
    total = e_rows[0]
    for r in range(1, rows):
        total = total + e_rows[r]
    e_out[...] = total
    gather.finish()
    for copy in across + keep:
        copy.wait()


def block_products(
    rows, cols, right_lane, with_trace, lmeta, rmeta, left, right, *rest
):
    if with_trace:
        out, e_out = rest[:2]
    else:
        e_in, out, e_out = rest[:3]
    acc, lbuf, rbuf, head, nxt, inner, mask, table, ml, mr, ms, sems = rest[-12:]
    slots = out.shape[0]
    i, j = lax.axis_index("row"), lax.axis_index("col")
    nblk = rows * TILE
    tile_cols = nblk // cols
    words = -(-nblk // 32)
    count_lane = 4 * slots
    acc[...] = jnp.zeros_like(acc)

    for t in range(TILE):
        head[t] = -1

    for t in range(tile_cols * words):
        mask[t] = 0

    @pl.loop(0, cols)
    def _(c):
        @pl.loop(0, lmeta[c, 0, count_lane])
        def _(s):
            row = lmeta[c, 0, s] - i * TILE
            idx = c * slots + s
            inner[idx] = lmeta[c, 0, slots + s]
            nxt[idx] = head[row]
            head[row] = idx

    @pl.loop(0, rows)
    def _(r):
        @pl.loop(0, rmeta[r, 0, count_lane + (1 if right_lane else 0)])
        def _(s):
            k = rmeta[r, 0, right_lane + s]
            col = rmeta[r, 0, right_lane + slots + s] - j * tile_cols
            word = col * words + (k >> 5)
            mask[word] = mask[word] | (jnp.int32(1) << (k & 31))
            table[k * tile_cols + col] = r * slots + s

    def find_slot(s, n):
        row = lmeta[j, 0, s] - i * TILE
        col = lmeta[j, 0, slots + s] - j * tile_cols

        def more(state):
            return state[0] >= 0

        def step(state):
            at, n = state
            k = inner[at]
            ml[n] = at
            mr[n] = table[k * tile_cols + col]
            ms[n] = s
            return nxt[at], n + ((mask[col * words + (k >> 5)] >> (k & 31)) & 1)

        return lax.while_loop(more, step, (head[row], n))[1]

    own_count = lmeta[j, 0, count_lane]
    found = lax.fori_loop(0, own_count, find_slot, jnp.int32(0))

    def fetch(base, m):
        a, b = ml[base + m], mr[base + m]
        return (
            pltpu.make_async_copy(left.at[a], lbuf.at[m], sems.at[0, m]),
            pltpu.make_async_copy(right.at[b], rbuf.at[m], sems.at[1, m]),
        )

    @pl.loop(0, (found + IN_FLIGHT - 1) // IN_FLIGHT)
    def _(chunk):
        base = chunk * IN_FLIGHT
        size = jnp.minimum(found - base, IN_FLIGHT)

        @pl.loop(0, size)
        def _(m):
            for copy in fetch(base, m):
                copy.start()

        @pl.loop(0, size)
        def _(m):
            for copy in fetch(base, m):
                copy.wait()
            s = ms[base + m]
            acc[s] += jnp.dot(lbuf[m], rbuf[m], preferred_element_type=jnp.float32)

    out[...] = acc[...].astype(out.dtype)
    if with_trace:
        size = acc.shape[1]
        e_out[...] = jnp.zeros_like(e_out)
        diagonal = lax.broadcasted_iota(jnp.int32, (size, size), 0) == lax.broadcasted_iota(
            jnp.int32, (size, size), 1
        )

        @pl.loop(0, own_count)
        def _(s):
            @pl.when(lmeta[j, 0, s] == lmeta[j, 0, slots + s])
            def _():
                e_out[...] += jnp.sum(jnp.where(diagonal, acc[s], 0.0))
    else:
        e_out[0, 0] = e_in[0, 0]


def per_device(rows, cols, p_values, p_where, p_count, h_values, h_where, h_count):
    slots, size, _ = p_values.shape
    dtype = p_values.dtype
    nblk = rows * TILE
    tile_cols = nblk // cols
    words = -(-nblk // 32)
    meta = jnp.concatenate(
        [p_where[:, 0], p_where[:, 1], h_where[:, 0], h_where[:, 1], p_count[0], h_count[0]]
    )
    meta = jnp.broadcast_to(jnp.pad(meta, (0, 128 - meta.shape[0]))[None, :], (8, 128))
    dma = pltpu.SemaphoreType.DMA
    chunks = CHUNKS if slots % CHUNKS == 0 else 1
    chunk_sems = [pltpu.VMEM((rows, slots, size, size), dtype)] + [dma((rows, chunks))] * 5
    col_sems = [dma((cols,)), dma((cols,))]
    row_sems = [dma((rows,)), dma((rows,))]
    tile = (slots, size, size)
    prow, hcol, prow_meta, col_meta = pl.pallas_call(
        functools.partial(first_gather, rows, cols),
        out_shape=[
            jax.ShapeDtypeStruct((cols,) + tile, dtype),
            jax.ShapeDtypeStruct((rows,) + tile, dtype),
            jax.ShapeDtypeStruct((cols, 8, 128), jnp.int32),
            jax.ShapeDtypeStruct((rows, 8, 128), jnp.int32),
        ],
        in_specs=[VMEM] * 3,
        out_specs=[ANY] * 4,
        scratch_shapes=chunk_sems + col_sems + col_sems + row_sems + [dma((4,))],
        compiler_params=pltpu.CompilerParams(collective_id=0, has_side_effects=True),
        name="first_gather",
    )(p_values, h_values, meta)

    def products(right_lane, with_trace, lmeta, rmeta, left, right, *more):
        smem = lambda n: pltpu.SMEM((n,), jnp.int32)
        most = slots * nblk + 1
        return pl.pallas_call(
            functools.partial(block_products, rows, cols, right_lane, with_trace),
            out_shape=[
                jax.ShapeDtypeStruct(tile, dtype),
                jax.ShapeDtypeStruct((8, 128) if with_trace else (1, 1), jnp.float32),
            ],
            in_specs=[SMEM, SMEM, ANY, ANY] + [SMEM] * len(more),
            out_specs=[VMEM, VMEM if with_trace else SMEM],
            scratch_shapes=[
                pltpu.VMEM(tile, jnp.float32),
                pltpu.VMEM((IN_FLIGHT, size, size), dtype),
                pltpu.VMEM((IN_FLIGHT, size, size), dtype),
                smem(TILE),
                smem(cols * slots),
                smem(cols * slots),
                smem(tile_cols * words),
                smem(nblk * tile_cols),
                smem(most),
                smem(most),
                smem(most),
                dma((2, IN_FLIGHT)),
            ],
            name="products",
        )(
            lmeta,
            rmeta,
            left.reshape((cols * slots, size, size)),
            right.reshape((rows * slots, size, size)),
            *more,
        )

    ph_values, part = products(2 * slots, True, prow_meta, col_meta, prow, hcol)
    frow, pcol, energy = pl.pallas_call(
        functools.partial(second_gather, rows, cols),
        out_shape=[
            jax.ShapeDtypeStruct((cols,) + tile, dtype),
            jax.ShapeDtypeStruct((rows,) + tile, dtype),
            jax.ShapeDtypeStruct((8, 128), jnp.float32),
        ],
        in_specs=[VMEM] * 3,
        out_specs=[ANY, ANY, VMEM],
        scratch_shapes=[
            pltpu.VMEM((cols, 8, 128), jnp.float32),
            pltpu.VMEM((rows, 8, 128), jnp.float32),
            pltpu.VMEM((8, 128), jnp.float32),
        ]
        + chunk_sems + col_sems + col_sems + row_sems + [dma((2,))],
        compiler_params=pltpu.CompilerParams(collective_id=1, has_side_effects=True),
        name="second_gather",
    )(p_values, ph_values, part)
    php_values, energy = products(0, False, prow_meta, col_meta, frow, pcol, energy)
    return (ph_values, php_values, energy[0, 0])


def solution(mesh):
    placed = (
        P("row", "col", None),
        P("row", "col"),
        P("row", "col"),
        P("row", "col", None),
        P("row", "col"),
        P("row", "col"),
    )
    return jax.shard_map(
        functools.partial(per_device, mesh.shape["row"], mesh.shape["col"]),
        mesh=mesh,
        in_specs=placed,
        out_specs=(P("row", "col", None), P("row", "col", None), P()),
        check_vma=False,
    )
```

```python
import functools

import jax
import jax.numpy as jnp
from jax import lax
from jax.experimental import pallas as pl
from jax.experimental.pallas import tpu as pltpu
from jax.sharding import PartitionSpec as P

TILE = 8
CHUNKS = 6
IN_FLIGHT = 16
MESH = pl.DeviceIdType.MESH
ANY = pl.BlockSpec(memory_space=pl.ANY)
VMEM = pl.BlockSpec(memory_space=pltpu.VMEM)
SMEM = pl.BlockSpec(memory_space=pltpu.SMEM)


def at_row(r):
    return (r, lax.axis_index("col"))


def at_col(c):
    return (lax.axis_index("row"), c)


def remote(src, dst, send_sem, recv_sem, device):
    return pltpu.make_async_remote_copy(
        src_ref=src,
        dst_ref=dst,
        send_sem=send_sem,
        recv_sem=recv_sem,
        device_id=device,
        device_id_type=MESH,
    )


def greet(rows, cols):
    me_row, me_col = lax.axis_index("row"), lax.axis_index("col")
    barrier = pltpu.get_barrier_semaphore()
    for d in range(1, rows):
        pl.semaphore_signal(
            barrier, inc=1, device_id=at_row((me_row + d) % rows), device_id_type=MESH
        )
    for d in range(1, cols):
        pl.semaphore_signal(
            barrier, inc=1, device_id=at_col((me_col + d) % cols), device_id_type=MESH
        )
    pl.semaphore_wait(barrier, rows + cols - 2)


class ColumnGather:
    def __init__(self, rows, own, land, out, up_send, down_send, x_send, recv, local):
        self.own, self.land, self.out = own, land, out
        self.up_send, self.down_send, self.x_send = up_send, down_send, x_send
        self.recv, self.local = recv, local
        self.inner = 2 if rows % 2 == 0 else 1
        self.outer = rows // self.inner
        self.chunks = recv.shape[1]
        self.size = own.shape[0] // self.chunks
        self.me = lax.axis_index("row")
        self.x, self.z = self.me % self.inner, self.me // self.inner
        self.cross_first = 1 if self.inner == 2 and self.chunks > 1 else 0

    def later(self, ch):
        return (ch + self.cross_first) % self.chunks

    def row(self, z, line):
        return z * self.inner + (self.x if line == 0 else self.inner - 1 - self.x)

    def part(self, ch):
        return pl.ds(ch * self.size, self.size)

    def copy(self, r, ch, own, way):
        sems, target = {
            "up": (self.up_send, self.me + self.inner),
            "down": (self.down_send, self.me - self.inner),
            "x": (self.x_send, self.row(self.z, 1)),
        }[way]
        part = self.part(ch)
        src = self.own.at[part] if own else self.land.at[r, part]
        return remote(src, self.land.at[r, part], sems.at[r, ch], self.recv.at[r, ch], at_row(target))

    def keep(self, r, ch):
        part = self.part(ch)
        return pltpu.make_async_copy(self.land.at[r, part], self.out.at[r, part], self.local.at[r, ch])

    def along(self, r, ch, own, act):
        @pl.when(self.z < self.outer - 1)
        def _():
            act(self.copy(r, ch, own, "up"))

        @pl.when(self.z > 0)
        def _():
            act(self.copy(r, ch, own, "down"))

    def arrive(self, r, ch):
        self.copy(r, ch, False, "x").wait_recv()
        self.keep(r, ch).start()

    def start(self):
        for ch in range(self.chunks):
            if self.inner == 2:
                self.copy(self.me, ch, True, "x").start()
            self.along(self.me, self.later(ch), True, lambda copy: copy.start())
        if self.cross_first:
            r = self.row(self.z, 1)
            self.arrive(r, 0)
            self.along(r, 0, False, lambda copy: copy.start())

    def pieces(self):
        lines = [(self.later(ch), 0) for ch in range(self.chunks)]
        return lines + [(0, 1)] * self.cross_first

    def relayed(self, d, side, ch, line, act):
        z = self.z - d if side == 0 else self.z + d
        there = self.z >= d if side == 0 else self.z + d < self.outer
        r = self.row(z, line)

        @pl.when(there)
        def _():
            if act == "start":
                self.arrive(r, ch)
            on = self.z < self.outer - 1 if side == 0 else self.z > 0

            @pl.when(on)
            def _():
                copy = self.copy(r, ch, False, "up" if side == 0 else "down")
                copy.start() if act == "start" else copy.wait_send()

            if self.inner == 2 and ch >= self.cross_first:
                copy = self.copy(r, ch, False, "x")
                copy.start() if act == "start" else copy.wait_send()

    def relay(self, d):
        for ch, line in self.pieces():
            for side in range(2):
                self.relayed(d, side, ch, line, "start")

    def finish(self):
        if self.inner == 2:
            for ch in range(self.cross_first, self.chunks):
                self.arrive(self.row(self.z, 1), ch)
            for d in range(1, self.outer):
                for side in range(2):
                    z = self.z - d if side == 0 else self.z + d
                    there = self.z >= d if side == 0 else self.z + d < self.outer

                    @pl.when(there)
                    def _():
                        for ch in range(self.cross_first, self.chunks):
                            self.arrive(self.row(z, 1), ch)
        for ch in range(self.chunks):
            if self.inner == 2:
                self.copy(self.me, ch, True, "x").wait_send()
            self.along(self.me, ch, True, lambda copy: copy.wait_send())
        if self.cross_first:
            self.along(self.row(self.z, 1), 0, False, lambda copy: copy.wait_send())
        for d in range(1, self.outer):
            for ch, line in self.pieces():
                for side in range(2):
                    self.relayed(d, side, ch, line, "wait")
        for r in range(self.inner * self.outer):
            @pl.when(r != self.me)
            def _():
                for ch in range(self.chunks):
                    self.keep(r, ch).wait()


def col_copies(cols, own, out, send, recv):
    me = lax.axis_index("col")
    made = []
    for d in range(1, cols):
        made.append(
            remote(own, out.at[me], send.at[d], recv.at[d], at_col((me + d) % cols))
        )
    return made


def row_copies(rows, own, out, send, recv):
    me = lax.axis_index("row")
    made = []
    for d in range(1, rows):
        made.append(
            remote(own, out.at[me], send.at[d], recv.at[d], at_row((me + d) % rows))
        )
    return made


def first_gather(
    rows, cols, p_ref, h_ref, meta_ref, prow, hcol, prow_meta, col_meta,
    land, up_send, down_send, x_send, recv, out_sems,
    p_send, p_recv, mc_send, mc_recv, mr_send, mr_recv, local,
):
    me_row, me_col = lax.axis_index("row"), lax.axis_index("col")
    keep = [
        pltpu.make_async_copy(h_ref, hcol.at[me_row], local.at[0]),
        pltpu.make_async_copy(p_ref, prow.at[me_col], local.at[1]),
        pltpu.make_async_copy(meta_ref, prow_meta.at[me_col], local.at[2]),
        pltpu.make_async_copy(meta_ref, col_meta.at[me_row], local.at[3]),
    ]
    greet(rows, cols)
    gather = ColumnGather(
        rows, h_ref, land, hcol, up_send, down_send, x_send, recv, out_sems
    )
    across = (
        col_copies(cols, p_ref, prow, p_send, p_recv)
        + col_copies(cols, meta_ref, prow_meta, mc_send, mc_recv)
        + row_copies(rows, meta_ref, col_meta, mr_send, mr_recv)
    )
    for copy in across + keep:
        copy.start()
    gather.start()
    for d in range(1, gather.outer):
        gather.relay(d)
    gather.finish()
    for copy in across + keep:
        copy.wait()


def second_gather(
    rows, cols, p_ref, f_ref, e_ref, frow, pcol, e_out,
    e_cols, e_rows, e_sum,
    land, up_send, down_send, x_send, recv, out_sems,
    p_send, p_recv, ec_send, ec_recv, er_send, er_recv, local,
):
    me_row, me_col = lax.axis_index("row"), lax.axis_index("col")
    keep = [
        pltpu.make_async_copy(p_ref, pcol.at[me_row], local.at[0]),
        pltpu.make_async_copy(f_ref, frow.at[me_col], local.at[1]),
    ]
    greet(rows, cols)
    energies = col_copies(cols, e_ref, e_cols, ec_send, ec_recv)
    for copy in energies:
        copy.start()
    gather = ColumnGather(
        rows, p_ref, land, pcol, up_send, down_send, x_send, recv, out_sems
    )
    across = col_copies(cols, f_ref, frow, p_send, p_recv)
    for copy in across + keep:
        copy.start()
    gather.start()
    e_cols[me_col] = e_ref[...]
    for copy in energies:
        copy.wait()
    total = e_cols[0]
    for c in range(1, cols):
        total = total + e_cols[c]
    e_sum[...] = total
    e_rows[me_row] = total
    if gather.outer > 1:
        gather.relay(1)
    sums = row_copies(rows, e_sum, e_rows, er_send, er_recv)
    for copy in sums:
        copy.start()
    for d in range(2, gather.outer):
        gather.relay(d)
    for copy in sums:
        copy.wait()
    total = e_rows[0]
    for r in range(1, rows):
        total = total + e_rows[r]
    e_out[...] = total
    gather.finish()
    for copy in across + keep:
        copy.wait()


def block_products(
    rows, cols, right_lane, with_trace, lmeta, rmeta, left, right, *rest
):
    if with_trace:
        out, e_out = rest[:2]
    else:
        e_in, out, e_out = rest[:3]
    acc, lbuf, rbuf, head, nxt, inner, mask, table, ml, mr, ms, sems = rest[-12:]
    slots = out.shape[0]
    i, j = lax.axis_index("row"), lax.axis_index("col")
    nblk = rows * TILE
    tile_cols = nblk // cols
    words = -(-nblk // 32)
    count_lane = 4 * slots
    acc[...] = jnp.zeros_like(acc)

    for t in range(TILE + 1):
        head[t] = -1

    for t in range(tile_cols * words + 1):
        mask[t] = 0

    @pl.loop(0, cols)
    def _(c):
        live = lmeta[c, 0, count_lane]
        for s in range(slots):
            row = jnp.where(s < live, lmeta[c, 0, s] - i * TILE, TILE)
            idx = c * slots + s
            inner[idx] = lmeta[c, 0, slots + s]
            nxt[idx] = head[row]
            head[row] = idx

    @pl.loop(0, rows)
    def _(r):
        live = rmeta[r, 0, count_lane + (1 if right_lane else 0)]
        for s in range(slots):
            k = rmeta[r, 0, right_lane + s]
            col = rmeta[r, 0, right_lane + slots + s] - j * tile_cols
            word = jnp.where(s < live, col * words + (k >> 5), tile_cols * words)
            mask[word] = mask[word] | (jnp.int32(1) << (k & 31))
            table[jnp.where(s < live, k * tile_cols + col, nblk * tile_cols)] = r * slots + s

    def find_slot(s, n):
        row = lmeta[j, 0, s] - i * TILE
        col = lmeta[j, 0, slots + s] - j * tile_cols

        def more(state):
            return state[0] >= 0

        def step(state):
            at, n = state
            k = inner[at]
            ml[n] = at
            mr[n] = table[k * tile_cols + col]
            ms[n] = s
            return nxt[at], n + ((mask[col * words + (k >> 5)] >> (k & 31)) & 1)

        return lax.while_loop(more, step, (head[row], n))[1]

    own_count = lmeta[j, 0, count_lane]
    found = lax.fori_loop(0, own_count, find_slot, jnp.int32(0))

    def fetch(base, m):
        a, b = ml[base + m], mr[base + m]
        return (
            pltpu.make_async_copy(left.at[a], lbuf.at[m], sems.at[0, m]),
            pltpu.make_async_copy(right.at[b], rbuf.at[m], sems.at[1, m]),
        )

    @pl.loop(0, (found + IN_FLIGHT - 1) // IN_FLIGHT)
    def _(chunk):
        base = chunk * IN_FLIGHT
        size = jnp.minimum(found - base, IN_FLIGHT)

        @pl.loop(0, size)
        def _(m):
            for copy in fetch(base, m):
                copy.start()

        @pl.loop(0, size)
        def _(m):
            for copy in fetch(base, m):
                copy.wait()
            s = ms[base + m]
            acc[s] += jnp.dot(lbuf[m], rbuf[m], preferred_element_type=jnp.float32)

    out[...] = acc[...].astype(out.dtype)
    if with_trace:
        size = acc.shape[1]
        e_out[...] = jnp.zeros_like(e_out)
        diagonal = lax.broadcasted_iota(jnp.int32, (size, size), 0) == lax.broadcasted_iota(
            jnp.int32, (size, size), 1
        )

        @pl.loop(0, own_count)
        def _(s):
            @pl.when(lmeta[j, 0, s] == lmeta[j, 0, slots + s])
            def _():
                e_out[...] += jnp.sum(jnp.where(diagonal, acc[s], 0.0))
    else:
        e_out[0, 0] = e_in[0, 0]


def per_device(rows, cols, p_values, p_where, p_count, h_values, h_where, h_count):
    slots, size, _ = p_values.shape
    dtype = p_values.dtype
    nblk = rows * TILE
    tile_cols = nblk // cols
    words = -(-nblk // 32)
    meta = jnp.concatenate(
        [p_where[:, 0], p_where[:, 1], h_where[:, 0], h_where[:, 1], p_count[0], h_count[0]]
    )
    meta = jnp.broadcast_to(jnp.pad(meta, (0, 128 - meta.shape[0]))[None, :], (8, 128))
    dma = pltpu.SemaphoreType.DMA
    chunks = CHUNKS if slots % CHUNKS == 0 else 1
    chunk_sems = [pltpu.VMEM((rows, slots, size, size), dtype)] + [dma((rows, chunks))] * 5
    col_sems = [dma((cols,)), dma((cols,))]
    row_sems = [dma((rows,)), dma((rows,))]
    tile = (slots, size, size)
    prow, hcol, prow_meta, col_meta = pl.pallas_call(
        functools.partial(first_gather, rows, cols),
        out_shape=[
            jax.ShapeDtypeStruct((cols,) + tile, dtype),
            jax.ShapeDtypeStruct((rows,) + tile, dtype),
            jax.ShapeDtypeStruct((cols, 8, 128), jnp.int32),
            jax.ShapeDtypeStruct((rows, 8, 128), jnp.int32),
        ],
        in_specs=[VMEM] * 3,
        out_specs=[ANY] * 4,
        scratch_shapes=chunk_sems + col_sems + col_sems + row_sems + [dma((4,))],
        compiler_params=pltpu.CompilerParams(collective_id=0, has_side_effects=True),
        name="first_gather",
    )(p_values, h_values, meta)

    def products(right_lane, with_trace, lmeta, rmeta, left, right, *more):
        smem = lambda n: pltpu.SMEM((n,), jnp.int32)
        most = slots * nblk + 1
        return pl.pallas_call(
            functools.partial(block_products, rows, cols, right_lane, with_trace),
            out_shape=[
                jax.ShapeDtypeStruct(tile, dtype),
                jax.ShapeDtypeStruct((8, 128) if with_trace else (1, 1), jnp.float32),
            ],
            in_specs=[SMEM, SMEM, ANY, ANY] + [SMEM] * len(more),
            out_specs=[VMEM, VMEM if with_trace else SMEM],
            scratch_shapes=[
                pltpu.VMEM(tile, jnp.float32),
                pltpu.VMEM((IN_FLIGHT, size, size), dtype),
                pltpu.VMEM((IN_FLIGHT, size, size), dtype),
                smem(TILE + 1),
                smem(cols * slots),
                smem(cols * slots),
                smem(tile_cols * words + 1),
                smem(nblk * tile_cols + 1),
                smem(most),
                smem(most),
                smem(most),
                dma((2, IN_FLIGHT)),
            ],
            name="products",
        )(
            lmeta,
            rmeta,
            left.reshape((cols * slots, size, size)),
            right.reshape((rows * slots, size, size)),
            *more,
        )

    ph_values, part = products(2 * slots, True, prow_meta, col_meta, prow, hcol)
    frow, pcol, energy = pl.pallas_call(
        functools.partial(second_gather, rows, cols),
        out_shape=[
            jax.ShapeDtypeStruct((cols,) + tile, dtype),
            jax.ShapeDtypeStruct((rows,) + tile, dtype),
            jax.ShapeDtypeStruct((8, 128), jnp.float32),
        ],
        in_specs=[VMEM] * 3,
        out_specs=[ANY, ANY, VMEM],
        scratch_shapes=[
            pltpu.VMEM((cols, 8, 128), jnp.float32),
            pltpu.VMEM((rows, 8, 128), jnp.float32),
            pltpu.VMEM((8, 128), jnp.float32),
        ]
        + chunk_sems + col_sems + col_sems + row_sems + [dma((2,))],
        compiler_params=pltpu.CompilerParams(collective_id=1, has_side_effects=True),
        name="second_gather",
    )(p_values, ph_values, part)
    php_values, energy = products(0, False, prow_meta, col_meta, frow, pcol, energy)
    return (ph_values, php_values, energy[0, 0])


def solution(mesh):
    placed = (
        P("row", "col", None),
        P("row", "col"),
        P("row", "col"),
        P("row", "col", None),
        P("row", "col"),
        P("row", "col"),
    )
    return jax.shard_map(
        functools.partial(per_device, mesh.shape["row"], mesh.shape["col"]),
        mesh=mesh,
        in_specs=placed,
        out_specs=(P("row", "col", None), P("row", "col", None), P()),
        check_vma=False,
    )
```

```python
import functools

import jax
import jax.numpy as jnp
from jax import lax
from jax.experimental import pallas as pl
from jax.experimental.pallas import tpu as pltpu
from jax.sharding import PartitionSpec as P

TILE = 8
CHUNKS = 12
IN_FLIGHT = 16
MESH = pl.DeviceIdType.MESH
ANY = pl.BlockSpec(memory_space=pl.ANY)
VMEM = pl.BlockSpec(memory_space=pltpu.VMEM)
SMEM = pl.BlockSpec(memory_space=pltpu.SMEM)


def at_row(r):
    return (r, lax.axis_index("col"))


def at_col(c):
    return (lax.axis_index("row"), c)


def remote(src, dst, send_sem, recv_sem, device):
    return pltpu.make_async_remote_copy(
        src_ref=src,
        dst_ref=dst,
        send_sem=send_sem,
        recv_sem=recv_sem,
        device_id=device,
        device_id_type=MESH,
    )


def greet(rows, cols):
    me_row, me_col = lax.axis_index("row"), lax.axis_index("col")
    barrier = pltpu.get_barrier_semaphore()
    for d in range(1, rows):
        pl.semaphore_signal(
            barrier, inc=1, device_id=at_row((me_row + d) % rows), device_id_type=MESH
        )
    for d in range(1, cols):
        pl.semaphore_signal(
            barrier, inc=1, device_id=at_col((me_col + d) % cols), device_id_type=MESH
        )
    pl.semaphore_wait(barrier, rows + cols - 2)


class ColumnGather:
    def __init__(self, rows, own, land, out, up_send, down_send, x_send, recv, local):
        self.own, self.land, self.out = own, land, out
        self.up_send, self.down_send, self.x_send = up_send, down_send, x_send
        self.recv, self.local = recv, local
        self.inner = 2 if rows % 2 == 0 else 1
        self.outer = rows // self.inner
        self.chunks = recv.shape[1]
        self.size = own.shape[0] // self.chunks
        self.me = lax.axis_index("row")
        self.x, self.z = self.me % self.inner, self.me // self.inner
        self.cross_first = self.chunks // 6 if self.inner == 2 else 0

    def later(self, ch):
        return (ch + self.cross_first) % self.chunks

    def row(self, z, line):
        return z * self.inner + (self.x if line == 0 else self.inner - 1 - self.x)

    def part(self, ch):
        return pl.ds(ch * self.size, self.size)

    def copy(self, r, ch, own, way):
        sems, target = {
            "up": (self.up_send, self.me + self.inner),
            "down": (self.down_send, self.me - self.inner),
            "x": (self.x_send, self.row(self.z, 1)),
        }[way]
        part = self.part(ch)
        src = self.own.at[part] if own else self.land.at[r, part]
        return remote(src, self.land.at[r, part], sems.at[r, ch], self.recv.at[r, ch], at_row(target))

    def keep(self, r, ch):
        part = self.part(ch)
        return pltpu.make_async_copy(self.land.at[r, part], self.out.at[r, part], self.local.at[r, ch])

    def along(self, r, ch, own, act):
        @pl.when(self.z < self.outer - 1)
        def _():
            act(self.copy(r, ch, own, "up"))

        @pl.when(self.z > 0)
        def _():
            act(self.copy(r, ch, own, "down"))

    def arrive(self, r, ch):
        self.copy(r, ch, False, "x").wait_recv()
        self.keep(r, ch).start()

    def start(self):
        for ch in range(self.chunks):
            if self.inner == 2:
                self.copy(self.me, ch, True, "x").start()
            self.along(self.me, self.later(ch), True, lambda copy: copy.start())
        for ch in range(self.cross_first):
            r = self.row(self.z, 1)
            self.arrive(r, ch)
            self.along(r, ch, False, lambda copy: copy.start())

    def pieces(self):
        lines = [(self.later(ch), 0) for ch in range(self.chunks)]
        return lines + [(ch, 1) for ch in range(self.cross_first)]

    def relayed(self, d, side, ch, line, act):
        z = self.z - d if side == 0 else self.z + d
        there = self.z >= d if side == 0 else self.z + d < self.outer
        r = self.row(z, line)

        @pl.when(there)
        def _():
            if act == "start":
                self.arrive(r, ch)
            on = self.z < self.outer - 1 if side == 0 else self.z > 0

            @pl.when(on)
            def _():
                copy = self.copy(r, ch, False, "up" if side == 0 else "down")
                copy.start() if act == "start" else copy.wait_send()

            if self.inner == 2 and ch >= self.cross_first:
                copy = self.copy(r, ch, False, "x")
                copy.start() if act == "start" else copy.wait_send()

    def relay(self, d):
        for ch, line in self.pieces():
            for side in range(2):
                self.relayed(d, side, ch, line, "start")

    def finish(self):
        if self.inner == 2:
            for ch in range(self.cross_first, self.chunks):
                self.arrive(self.row(self.z, 1), ch)
            for d in range(1, self.outer):
                for side in range(2):
                    z = self.z - d if side == 0 else self.z + d
                    there = self.z >= d if side == 0 else self.z + d < self.outer

                    @pl.when(there)
                    def _():
                        for ch in range(self.cross_first, self.chunks):
                            self.arrive(self.row(z, 1), ch)
        for ch in range(self.chunks):
            if self.inner == 2:
                self.copy(self.me, ch, True, "x").wait_send()
            self.along(self.me, ch, True, lambda copy: copy.wait_send())
        for ch in range(self.cross_first):
            self.along(self.row(self.z, 1), ch, False, lambda copy: copy.wait_send())
        for d in range(1, self.outer):
            for ch, line in self.pieces():
                for side in range(2):
                    self.relayed(d, side, ch, line, "wait")
        for r in range(self.inner * self.outer):
            @pl.when(r != self.me)
            def _():
                for ch in range(self.chunks):
                    self.keep(r, ch).wait()


def col_copies(cols, own, out, send, recv):
    me = lax.axis_index("col")
    made = []
    for d in range(1, cols):
        made.append(
            remote(own, out.at[me], send.at[d], recv.at[d], at_col((me + d) % cols))
        )
    return made


def row_copies(rows, own, out, send, recv):
    me = lax.axis_index("row")
    made = []
    for d in range(1, rows):
        made.append(
            remote(own, out.at[me], send.at[d], recv.at[d], at_row((me + d) % rows))
        )
    return made


def first_gather(
    rows, cols, p_ref, h_ref, meta_ref, prow, hcol, prow_meta, col_meta,
    land, up_send, down_send, x_send, recv, out_sems,
    p_send, p_recv, mc_send, mc_recv, mr_send, mr_recv, local,
):
    me_row, me_col = lax.axis_index("row"), lax.axis_index("col")
    keep = [
        pltpu.make_async_copy(h_ref, hcol.at[me_row], local.at[0]),
        pltpu.make_async_copy(p_ref, prow.at[me_col], local.at[1]),
        pltpu.make_async_copy(meta_ref, prow_meta.at[me_col], local.at[2]),
        pltpu.make_async_copy(meta_ref, col_meta.at[me_row], local.at[3]),
    ]
    greet(rows, cols)
    gather = ColumnGather(
        rows, h_ref, land, hcol, up_send, down_send, x_send, recv, out_sems
    )
    across = (
        col_copies(cols, p_ref, prow, p_send, p_recv)
        + col_copies(cols, meta_ref, prow_meta, mc_send, mc_recv)
        + row_copies(rows, meta_ref, col_meta, mr_send, mr_recv)
    )
    for copy in across + keep:
        copy.start()
    gather.start()
    for d in range(1, gather.outer):
        gather.relay(d)
    gather.finish()
    for copy in across + keep:
        copy.wait()


def second_gather(
    rows, cols, p_ref, f_ref, e_ref, frow, pcol, e_out,
    e_cols, e_rows, e_sum,
    land, up_send, down_send, x_send, recv, out_sems,
    p_send, p_recv, ec_send, ec_recv, er_send, er_recv, local,
):
    me_row, me_col = lax.axis_index("row"), lax.axis_index("col")
    keep = [
        pltpu.make_async_copy(p_ref, pcol.at[me_row], local.at[0]),
        pltpu.make_async_copy(f_ref, frow.at[me_col], local.at[1]),
    ]
    greet(rows, cols)
    energies = col_copies(cols, e_ref, e_cols, ec_send, ec_recv)
    for copy in energies:
        copy.start()
    gather = ColumnGather(
        rows, p_ref, land, pcol, up_send, down_send, x_send, recv, out_sems
    )
    across = col_copies(cols, f_ref, frow, p_send, p_recv)
    for copy in across + keep:
        copy.start()
    gather.start()
    e_cols[me_col] = e_ref[...]
    for copy in energies:
        copy.wait()
    total = e_cols[0]
    for c in range(1, cols):
        total = total + e_cols[c]
    e_sum[...] = total
    e_rows[me_row] = total
    if gather.outer > 1:
        gather.relay(1)
    sums = row_copies(rows, e_sum, e_rows, er_send, er_recv)
    for copy in sums:
        copy.start()
    for d in range(2, gather.outer):
        gather.relay(d)
    for copy in sums:
        copy.wait()
    total = e_rows[0]
    for r in range(1, rows):
        total = total + e_rows[r]
    e_out[...] = total
    gather.finish()
    for copy in across + keep:
        copy.wait()


def block_products(
    rows, cols, right_lane, with_trace, lmeta, rmeta, left, right, *rest
):
    if with_trace:
        out, e_out = rest[:2]
    else:
        e_in, out, e_out = rest[:3]
    acc, lbuf, rbuf, head, nxt, inner, mask, table, ml, mr, ms, sems = rest[-12:]
    slots = out.shape[0]
    i, j = lax.axis_index("row"), lax.axis_index("col")
    nblk = rows * TILE
    tile_cols = nblk // cols
    words = -(-nblk // 32)
    count_lane = 4 * slots
    acc[...] = jnp.zeros_like(acc)

    for t in range(TILE + 1):
        head[t] = -1

    for t in range(tile_cols * words + 1):
        mask[t] = 0

    @pl.loop(0, cols)
    def _(c):
        live = lmeta[c, 0, count_lane]
        for s in range(slots):
            row = jnp.where(s < live, lmeta[c, 0, s] - i * TILE, TILE)
            idx = c * slots + s
            inner[idx] = lmeta[c, 0, slots + s]
            nxt[idx] = head[row]
            head[row] = idx

    @pl.loop(0, rows)
    def _(r):
        live = rmeta[r, 0, count_lane + (1 if right_lane else 0)]
        for s in range(slots):
            k = rmeta[r, 0, right_lane + s]
            col = rmeta[r, 0, right_lane + slots + s] - j * tile_cols
            word = jnp.where(s < live, col * words + (k >> 5), tile_cols * words)
            mask[word] = mask[word] | (jnp.int32(1) << (k & 31))
            table[jnp.where(s < live, k * tile_cols + col, nblk * tile_cols)] = r * slots + s

    def find_slot(s, n):
        row = lmeta[j, 0, s] - i * TILE
        col = lmeta[j, 0, slots + s] - j * tile_cols

        def more(state):
            return state[0] >= 0

        def step(state):
            at, n = state
            k = inner[at]
            ml[n] = at
            mr[n] = table[k * tile_cols + col]
            ms[n] = s
            return nxt[at], n + ((mask[col * words + (k >> 5)] >> (k & 31)) & 1)

        return lax.while_loop(more, step, (head[row], n))[1]

    own_count = lmeta[j, 0, count_lane]
    found = lax.fori_loop(0, own_count, find_slot, jnp.int32(0))

    def fetch(base, m):
        a, b = ml[base + m], mr[base + m]
        return (
            pltpu.make_async_copy(left.at[a], lbuf.at[m], sems.at[0, m]),
            pltpu.make_async_copy(right.at[b], rbuf.at[m], sems.at[1, m]),
        )

    @pl.loop(0, (found + IN_FLIGHT - 1) // IN_FLIGHT)
    def _(chunk):
        base = chunk * IN_FLIGHT
        size = jnp.minimum(found - base, IN_FLIGHT)

        @pl.loop(0, size)
        def _(m):
            for copy in fetch(base, m):
                copy.start()

        @pl.loop(0, size)
        def _(m):
            for copy in fetch(base, m):
                copy.wait()
            s = ms[base + m]
            acc[s] += jnp.dot(lbuf[m], rbuf[m], preferred_element_type=jnp.float32)

    out[...] = acc[...].astype(out.dtype)
    if with_trace:
        size = acc.shape[1]
        e_out[...] = jnp.zeros_like(e_out)
        diagonal = lax.broadcasted_iota(jnp.int32, (size, size), 0) == lax.broadcasted_iota(
            jnp.int32, (size, size), 1
        )

        @pl.loop(0, own_count)
        def _(s):
            @pl.when(lmeta[j, 0, s] == lmeta[j, 0, slots + s])
            def _():
                e_out[...] += jnp.sum(jnp.where(diagonal, acc[s], 0.0))
    else:
        e_out[0, 0] = e_in[0, 0]


def per_device(rows, cols, p_values, p_where, p_count, h_values, h_where, h_count):
    slots, size, _ = p_values.shape
    dtype = p_values.dtype
    nblk = rows * TILE
    tile_cols = nblk // cols
    words = -(-nblk // 32)
    meta = jnp.concatenate(
        [p_where[:, 0], p_where[:, 1], h_where[:, 0], h_where[:, 1], p_count[0], h_count[0]]
    )
    meta = jnp.broadcast_to(jnp.pad(meta, (0, 128 - meta.shape[0]))[None, :], (8, 128))
    dma = pltpu.SemaphoreType.DMA
    chunks = CHUNKS if slots % CHUNKS == 0 else 1
    chunk_sems = [pltpu.VMEM((rows, slots, size, size), dtype)] + [dma((rows, chunks))] * 5
    col_sems = [dma((cols,)), dma((cols,))]
    row_sems = [dma((rows,)), dma((rows,))]
    tile = (slots, size, size)
    prow, hcol, prow_meta, col_meta = pl.pallas_call(
        functools.partial(first_gather, rows, cols),
        out_shape=[
            jax.ShapeDtypeStruct((cols,) + tile, dtype),
            jax.ShapeDtypeStruct((rows,) + tile, dtype),
            jax.ShapeDtypeStruct((cols, 8, 128), jnp.int32),
            jax.ShapeDtypeStruct((rows, 8, 128), jnp.int32),
        ],
        in_specs=[VMEM] * 3,
        out_specs=[ANY] * 4,
        scratch_shapes=chunk_sems + col_sems + col_sems + row_sems + [dma((4,))],
        compiler_params=pltpu.CompilerParams(collective_id=0, has_side_effects=True),
        name="first_gather",
    )(p_values, h_values, meta)

    def products(right_lane, with_trace, lmeta, rmeta, left, right, *more):
        smem = lambda n: pltpu.SMEM((n,), jnp.int32)
        most = slots * nblk + 1
        return pl.pallas_call(
            functools.partial(block_products, rows, cols, right_lane, with_trace),
            out_shape=[
                jax.ShapeDtypeStruct(tile, dtype),
                jax.ShapeDtypeStruct((8, 128) if with_trace else (1, 1), jnp.float32),
            ],
            in_specs=[SMEM, SMEM, ANY, ANY] + [SMEM] * len(more),
            out_specs=[VMEM, VMEM if with_trace else SMEM],
            scratch_shapes=[
                pltpu.VMEM(tile, jnp.float32),
                pltpu.VMEM((IN_FLIGHT, size, size), dtype),
                pltpu.VMEM((IN_FLIGHT, size, size), dtype),
                smem(TILE + 1),
                smem(cols * slots),
                smem(cols * slots),
                smem(tile_cols * words + 1),
                smem(nblk * tile_cols + 1),
                smem(most),
                smem(most),
                smem(most),
                dma((2, IN_FLIGHT)),
            ],
            name="products",
        )(
            lmeta,
            rmeta,
            left.reshape((cols * slots, size, size)),
            right.reshape((rows * slots, size, size)),
            *more,
        )

    ph_values, part = products(2 * slots, True, prow_meta, col_meta, prow, hcol)
    frow, pcol, energy = pl.pallas_call(
        functools.partial(second_gather, rows, cols),
        out_shape=[
            jax.ShapeDtypeStruct((cols,) + tile, dtype),
            jax.ShapeDtypeStruct((rows,) + tile, dtype),
            jax.ShapeDtypeStruct((8, 128), jnp.float32),
        ],
        in_specs=[VMEM] * 3,
        out_specs=[ANY, ANY, VMEM],
        scratch_shapes=[
            pltpu.VMEM((cols, 8, 128), jnp.float32),
            pltpu.VMEM((rows, 8, 128), jnp.float32),
            pltpu.VMEM((8, 128), jnp.float32),
        ]
        + chunk_sems + col_sems + col_sems + row_sems + [dma((2,))],
        compiler_params=pltpu.CompilerParams(collective_id=1, has_side_effects=True),
        name="second_gather",
    )(p_values, ph_values, part)
    php_values, energy = products(0, False, prow_meta, col_meta, frow, pcol, energy)
    return (ph_values, php_values, energy[0, 0])


def solution(mesh):
    placed = (
        P("row", "col", None),
        P("row", "col"),
        P("row", "col"),
        P("row", "col", None),
        P("row", "col"),
        P("row", "col"),
    )
    return jax.shard_map(
        functools.partial(per_device, mesh.shape["row"], mesh.shape["col"]),
        mesh=mesh,
        in_specs=placed,
        out_specs=(P("row", "col", None), P("row", "col", None), P()),
        check_vma=False,
    )
```
